16 devices in a mesh: fsdp: 4 (over z, y), ep: 4 (over x, core).
Axes of the slice: x: 2, y: 2, z: 2, core: 2. Of those that a mesh axis runs over, the one named last changes fastest.
Arguments:
- x_in: bfloat16 [2, 16384, 896], P(None, ('fsdp', 'ep'))
- dy_out: bfloat16 [2, 16384, 896], P(None, ('fsdp', 'ep'))
- expert_idx: int32 [2, 16384, 8], P(None, ('fsdp', 'ep'))
- gate_prob: float32 [2, 16384, 8], P(None, ('fsdp', 'ep'))
- w_one: bfloat16 [64, 896, 640], P('ep', 'fsdp')
- w_two: bfloat16 [64, 640, 896], P('ep', None, 'fsdp')
- w_three: bfloat16 [64, 896, 640], P('ep', 'fsdp')
Outputs:
- output 1: bfloat16 [2, 16384, 896], P(None, ('fsdp', 'ep'))
- output 2: float32 [2, 16384, 8], P(None, ('fsdp', 'ep'))
- output 3: float32 [64, 896, 640], P('ep', 'fsdp')
- output 4: float32 [64, 640, 896], P('ep', None, 'fsdp')
- output 5: float32 [64, 896, 640], P('ep', 'fsdp')
All inputs are finite; a program needn't handle non-finite values.
Results may differ from the reference program's by a relative error of at most 0.0011.
Values are sent between devices in bfloat16 or wider.
A program may use at most 1 GiB of HBM per device.

```python
import jax
import jax.numpy as jnp
from jax import lax

D_MODEL = 896
FF_DIM = 640
EXPERTS = 64
TOP_K = 8
TOK_DEV = 1024
SOURCES = 16
MICRO_BATCHES = 2
CAPACITY = 160

TOKENS = SOURCES * TOK_DEV
N_CHOICE = TOK_DEV * TOP_K


def draw_routing(key):
    key_hot, key_bias, key_score = jax.random.split(key, 3)
    expert_ids = jnp.arange(EXPERTS, dtype=jnp.int32)
    hot_ids = jax.random.randint(key_hot, (MICRO_BATCHES, SOURCES, 1, 1), 0, EXPERTS)
    forced = jnp.arange(TOK_DEV)[:, None] < CAPACITY
    hot_bonus = jnp.where(expert_ids == hot_ids, 1, 0) * jnp.where(forced, 4096, 512)
    source_bias = jax.random.randint(key_bias, (MICRO_BATCHES, SOURCES, 1, EXPERTS), 0, 512)
    rand_score = jax.random.randint(key_score, (MICRO_BATCHES, SOURCES, TOK_DEV, EXPERTS), 0, 1024)
    total_score = (rand_score + source_bias + hot_bonus) * EXPERTS + expert_ids
    chosen = lax.top_k(total_score, TOP_K)[1]
    return chosen.reshape(MICRO_BATCHES, TOKENS, TOP_K).astype(jnp.int32)


def setup_inputs(seed: int = 0) -> dict:
    key_list = jax.random.split(jax.random.key(seed), 7)
    x_vals = jax.random.normal(key_list[0], (MICRO_BATCHES, TOKENS, D_MODEL), jnp.float32)
    dy_vals = jax.random.normal(key_list[1], (MICRO_BATCHES, TOKENS, D_MODEL), jnp.float32)
    routing = draw_routing(key_list[2])
    gate_vals = jax.random.uniform(key_list[3], (MICRO_BATCHES, TOKENS, TOP_K), jnp.float32, 0.2, 1.0)
    w_one = jax.random.normal(key_list[4], (EXPERTS, D_MODEL, FF_DIM), jnp.float32) * D_MODEL ** -0.5
    w_two = jax.random.normal(key_list[5], (EXPERTS, FF_DIM, D_MODEL), jnp.float32) * FF_DIM ** -0.5
    w_three = jax.random.normal(key_list[6], (EXPERTS, D_MODEL, FF_DIM), jnp.float32) * D_MODEL ** -0.5
    return {'x_in': x_vals.astype(jnp.bfloat16), 'dy_out': dy_vals.astype(jnp.bfloat16), 'expert_idx': routing, 'gate_prob': gate_vals, 'w_one': w_one.astype(jnp.bfloat16), 'w_two': w_two.astype(jnp.bfloat16), 'w_three': w_three.astype(jnp.bfloat16)}


def slot_holder(ids_flat):
    one_hot = (ids_flat[:, None] == jnp.arange(EXPERTS, dtype=jnp.int32)[None, :]).astype(jnp.int32)
    position = jnp.sum((jnp.cumsum(one_hot, axis=0) - one_hot) * one_hot, axis=1)
    choice_slot = jnp.where(position < CAPACITY, ids_flat * CAPACITY + position, EXPERTS * CAPACITY)
    holder = jnp.full((EXPERTS * CAPACITY + 1,), N_CHOICE, jnp.int32)
    holder = holder.at[choice_slot].set(jnp.arange(N_CHOICE, dtype=jnp.int32))
    return holder[:EXPERTS * CAPACITY]


def expert_rows(x_rows, dy_rows, gate_rows, w_a, w_b, w_c):
    h_one = jnp.dot(x_rows, w_a, preferred_element_type=jnp.float32)
    h_three = jnp.dot(x_rows, w_c, preferred_element_type=jnp.float32)
    sigma_one = jax.nn.sigmoid(h_one)
    silu_one = h_one * sigma_one
    act_bf = (silu_one * h_three).astype(jnp.bfloat16)
    y_rows = jnp.dot(act_bf, w_b, preferred_element_type=jnp.float32)
    dg_rows = jnp.sum(dy_rows.astype(jnp.float32) * y_rows, axis=1)
    g_rows = (gate_rows[:, None] * dy_rows.astype(jnp.float32)).astype(jnp.bfloat16)
    d_act = jnp.dot(g_rows, w_b.T, preferred_element_type=jnp.float32)
    dh_three = (d_act * silu_one).astype(jnp.bfloat16)
    dh_one = (d_act * h_three * sigma_one * (1.0 + h_one * (1.0 - sigma_one))).astype(jnp.bfloat16)
    dx_rows = (jnp.dot(dh_one, w_a.T, preferred_element_type=jnp.float32) + jnp.dot(dh_three, w_c.T, preferred_element_type=jnp.float32)).astype(jnp.bfloat16)
    gw_one = jnp.dot(x_rows.T, dh_one, preferred_element_type=jnp.float32)
    gw_two = jnp.dot(act_bf.T, g_rows, preferred_element_type=jnp.float32)
    gw_three = jnp.dot(x_rows.T, dh_three, preferred_element_type=jnp.float32)
    return dx_rows, dg_rows, gw_one, gw_two, gw_three


def reference(x_in, dy_out, expert_idx, gate_prob, w_one, w_two, w_three):
    total_choices = MICRO_BATCHES * TOKENS * TOP_K
    holder = lax.map(slot_holder, expert_idx.reshape(MICRO_BATCHES * SOURCES, N_CHOICE))
    block_base = jnp.arange(MICRO_BATCHES * SOURCES, dtype=jnp.int32)[:, None] * N_CHOICE
    slot_choice = jnp.where(holder < N_CHOICE, holder + block_base, total_choices)
    slot_choice = jnp.transpose(slot_choice.reshape(MICRO_BATCHES, SOURCES, EXPERTS, CAPACITY), (2, 0, 1, 3))
    slot_choice = slot_choice.reshape(EXPERTS, MICRO_BATCHES, SOURCES * CAPACITY)
    zero_row = jnp.zeros((1, D_MODEL), x_in.dtype)
    x_flat = jnp.concatenate([x_in.reshape(MICRO_BATCHES * TOKENS, D_MODEL), zero_row], axis=0)
    dy_flat = jnp.concatenate([dy_out.reshape(MICRO_BATCHES * TOKENS, D_MODEL), zero_row], axis=0)
    gate_flat = jnp.concatenate([gate_prob.reshape(total_choices), jnp.zeros((1,), gate_prob.dtype)])

    def expert_step(scan_state, per_expert):
        dx_acc, dg_acc = scan_state
        w_a, w_b, w_c, choices = per_expert
        grad_one = jnp.zeros((D_MODEL, FF_DIM), jnp.float32)
        grad_two = jnp.zeros((FF_DIM, D_MODEL), jnp.float32)
        grad_three = jnp.zeros((D_MODEL, FF_DIM), jnp.float32)
        for mb_index in range(MICRO_BATCHES):
            pick_ids = choices[mb_index]
            tok_ids = pick_ids // TOP_K
            dx_rows, dg_rows, gw_one, gw_two, gw_three = expert_rows(x_flat[tok_ids], dy_flat[tok_ids], gate_flat[pick_ids], w_a, w_b, w_c)
            dx_acc = dx_acc.at[tok_ids].add(dx_rows.astype(jnp.float32))
            dg_acc = dg_acc.at[pick_ids].set(dg_rows)
            grad_one = grad_one + gw_one
            grad_two = grad_two + gw_two
            grad_three = grad_three + gw_three
        return (dx_acc, dg_acc), (grad_one, grad_two, grad_three)

    start_state = (jnp.zeros((MICRO_BATCHES * TOKENS + 1, D_MODEL), jnp.float32), jnp.zeros((total_choices + 1,), jnp.float32))
    end_state, grad_stack = lax.scan(expert_step, start_state, (w_one, w_two, w_three, slot_choice))
    dx_in = end_state[0][:MICRO_BATCHES * TOKENS].astype(jnp.bfloat16).reshape(MICRO_BATCHES, TOKENS, D_MODEL)
    d_gate = end_state[1][:total_choices].reshape(MICRO_BATCHES, TOKENS, TOP_K)
    return (dx_in, d_gate, grad_stack[0], grad_stack[1], grad_stack[2])
```

```python
import functools

import jax
import jax.numpy as jnp
from jax import lax
from jax.experimental import pallas as pl
from jax.experimental.pallas import tpu as pltpu
from jax.sharding import Mesh, PartitionSpec as P


MICRO = 2
TOK = 1024
TOP_K = 8
D = 896
F = 640
CAP = 160
SRC = 8
EXP = 8
QUARTER = D // 4
HALF = D // 2
ROWS = SRC * CAP
CHUNK = 2
N_CHUNK = EXP // CHUNK
WIDE = 3 * F
TOKEN_ROWS = TOK + 16

BF16 = jnp.bfloat16
F32 = jnp.float32
VMEM_LIMIT = 62 * 1024 * 1024


def params(**kw):
    return pltpu.CompilerParams(vmem_limit_bytes=VMEM_LIMIT, **kw)


def routing_kernel(first_ref, ids_ref, gate_ref, pos_ref, gsel_ref, member):
    first = first_ref[0]
    for mb in range(MICRO):
        for src in range(SRC):
            ids = ids_ref[src, mb]
            gate = gate_ref[src, mb]
            for e in range(EXP):
                hit = ids == first + e
                row = (mb * SRC + src) * EXP + e
                member[row:row + 1, :] = jnp.sum(jnp.where(hit, 1.0, 0.0), axis=0, keepdims=True)
                gsel_ref[mb, src, e:e + 1, :] = jnp.sum(jnp.where(hit, gate, 0.0), axis=0, keepdims=True)
    earlier = lax.broadcasted_iota(jnp.int32, (TOK, TOK), 0) < lax.broadcasted_iota(jnp.int32, (TOK, TOK), 1)
    chosen = member[...]
    count = jnp.dot(chosen.astype(BF16), jnp.where(earlier, 1.0, 0.0).astype(BF16), preferred_element_type=F32)
    kept = (chosen > 0.5) & (count < CAP - 0.5)
    slot = jnp.where(kept, count, -1.0).astype(jnp.int32)
    pos_ref[...] = slot.reshape(MICRO, SRC, EXP, TOK)


def routing(first, ids, gate):
    shape = (MICRO, SRC, EXP, TOK)
    return pl.pallas_call(
        routing_kernel,
        out_shape=(jax.ShapeDtypeStruct(shape, jnp.int32), jax.ShapeDtypeStruct(shape, F32)),
        in_specs=[pl.BlockSpec(memory_space=pltpu.SMEM), pl.BlockSpec(memory_space=pltpu.VMEM), pl.BlockSpec(memory_space=pltpu.VMEM)],
        out_specs=(pl.BlockSpec(memory_space=pltpu.VMEM), pl.BlockSpec(memory_space=pltpu.VMEM)),
        scratch_shapes=[pltpu.VMEM((MICRO * SRC * EXP, TOK), F32)],
        compiler_params=params(),
        name="routing",
        cost_estimate=pl.CostEstimate(flops=2 * 128 * TOK * TOK, bytes_accessed=3 << 20, transcendentals=0),
    )(first, ids, gate)


def gather_kernel(tok_ref, pos_ref, gate_ref, x_ref, dy_ref, g_ref, pick, gcol):
    slots = lax.broadcasted_iota(jnp.int32, (CAP, TOK), 0)
    for e in range(EXP):
        hit = slots == pos_ref[e:e + 1, :]
        pick[e * CAP:(e + 1) * CAP, :] = jnp.where(hit, 1.0, 0.0).astype(BF16)
        col = jnp.sum(jnp.where(hit, gate_ref[e:e + 1, :], 0.0), axis=1, keepdims=True)
        gcol[e * CAP:(e + 1) * CAP, :] = jnp.broadcast_to(col, (CAP, 128))
    part = EXP // 2

    def body(c, carry):
        rows = pl.ds(pl.multiple_of(c * part * CAP, part * CAP), part * CAP)
        sel = pick[rows, :]
        x_rows = jnp.dot(sel, tok_ref[:TOK, :], preferred_element_type=F32)
        x_ref[pl.ds(c * part, part)] = x_rows.astype(BF16).reshape(part, CAP, D)
        dy_rows = jnp.dot(sel, tok_ref[TOK:, :], preferred_element_type=F32)
        dy_ref[pl.ds(c * part, part)] = dy_rows.astype(BF16).reshape(part, CAP, D)
        g_rows = (gcol[rows, :1] * dy_rows).astype(BF16)
        g_ref[pl.ds(c * part, part)] = g_rows.reshape(part, CAP, D)
        return carry

    lax.fori_loop(0, 2, body, 0)


def gather_rows(tokens, pos, gate, mb):
    rows = jax.ShapeDtypeStruct((EXP, ROWS, D), BF16)
    table = pl.BlockSpec((None, None, EXP, TOK), lambda s: (mb, s, 0, 0))
    out = pl.BlockSpec((EXP, CAP, D), lambda s: (0, s, 0))
    return pl.pallas_call(
        gather_kernel,
        grid=(SRC,),
        out_shape=(rows, rows, rows),
        in_specs=[pl.BlockSpec((None, 2 * TOK, D), lambda s: (s, 0, 0)), table, table],
        out_specs=(out, out, out),
        scratch_shapes=[pltpu.VMEM((ROWS, TOK), BF16), pltpu.VMEM((ROWS, 128), F32)],
        compiler_params=params(),
        name="gather_rows",
        cost_estimate=pl.CostEstimate(flops=4 * SRC * ROWS * TOK * D, bytes_accessed=90 << 20, transcendentals=0),
    )(tokens, pos, gate)


def expert_kernel(add_into, place_ref, x_ref, dy_ref, g_ref, own_ref, yr_ref, zo_ref, zf_ref, *refs):
    if add_into:
        acc_ref, dx_ref, dg_ref, keep_ref, send_ref = refs[:5]
        refs = refs[5:]
    else:
        dx_ref, dg_ref, part_ref = refs[:3]
        refs = refs[3:]
    w, act, dh, x_t, g_t, dw, w_sem, acc_sem, out_sem = refs
    i = pl.program_id(0)
    z, y = place_ref[0], place_ref[1]
    quarters = (2 * z + y, 2 * z + 1 - y, 2 * (1 - z) + y, 2 * (1 - z) + 1 - y)

    def weight_copies(j):
        return [
            pltpu.make_async_copy(ref.at[j], w.at[j, pl.ds(pl.multiple_of(q * QUARTER, QUARTER), QUARTER), :], w_sem.at[j])
            for ref, q in zip((own_ref, yr_ref, zo_ref, zf_ref), quarters)
        ]

    def out_copies(j):
        if not add_into:
            return [pltpu.make_async_copy(dw, part_ref.at[j], out_sem.at[0])]
        return [
            pltpu.make_async_copy(dw.at[pl.ds(pl.multiple_of(z * HALF, HALF), HALF), :], keep_ref.at[j], out_sem.at[0]),
            pltpu.make_async_copy(dw.at[pl.ds(pl.multiple_of((1 - z) * HALF, HALF), HALF), :], send_ref.at[j], out_sem.at[1]),
        ]

    @pl.when(i == 0)
    def _():
        for j in range(CHUNK):
            for copy in weight_copies(j):
                copy.start()

    @pl.when(i > 0)
    def _():
        for copy in out_copies(i - 1):
            copy.wait()

    if add_into:
        pltpu.make_async_copy(acc_ref.at[i], dw, acc_sem).start()
    for copy in weight_copies(i):
        copy.wait()

    part = ROWS // 2

    def body(c, carry):
        start = pl.multiple_of(c * part, part)
        rows = pl.ds(start, part)
        x_c = x_ref[rows, :]
        g_c = g_ref[rows, :]
        h = jnp.dot(x_c, w[i, :, :2 * F], preferred_element_type=F32)
        h_one = h[:, :F]
        h_three = h[:, F:]
        sigma = jax.nn.sigmoid(h_one)
        silu = h_one * sigma
        act_c = (silu * h_three).astype(BF16)
        act[rows, :] = act_c
        y_c = lax.dot_general(act_c, w[i, :, 2 * F:], (((1,), (1,)), ((), ())), preferred_element_type=F32)
        dg = jnp.sum(dy_ref[rows, :].astype(F32) * y_c, axis=1, keepdims=True)
        dg_ref[rows, :] = jnp.broadcast_to(dg, (part, 128))
        d_act = jnp.dot(g_c, w[i, :, 2 * F:], preferred_element_type=F32)
        dh_three = (d_act * silu).astype(BF16)
        dh_one = (d_act * h_three * sigma * (1.0 + h_one * (1.0 - sigma))).astype(BF16)
        dh[rows, :F] = dh_one
        dh[rows, F:] = dh_three
        dx = lax.dot_general(dh[rows, :], w[i, :, :2 * F], (((1,), (1,)), ((), ())), preferred_element_type=F32)
        dx_ref[rows, :] = dx.astype(BF16)
        x_t[:, rows] = x_c.T
        g_t[:, rows] = g_c.T
        return carry

    lax.fori_loop(0, 2, body, 0)
    if add_into:
        pltpu.make_async_copy(acc_ref.at[i], dw, acc_sem).wait()
        dw[:, :2 * F] += jnp.dot(x_t[...], dh[...], preferred_element_type=F32)
        dw[:, 2 * F:] += jnp.dot(g_t[...], act[...], preferred_element_type=F32)
    else:
        dw[:, :2 * F] = jnp.dot(x_t[...], dh[...], preferred_element_type=F32)
        dw[:, 2 * F:] = jnp.dot(g_t[...], act[...], preferred_element_type=F32)
    for copy in out_copies(i):
        copy.start()

    @pl.when(i == CHUNK - 1)
    def _():
        for copy in out_copies(i):
            copy.wait()


def run_experts(place, rows, pieces, acc, k):
    add_into = acc is not None
    row_in = pl.BlockSpec((None, ROWS, D), lambda i: (k * CHUNK + i, 0, 0))
    anywhere = pl.BlockSpec(memory_space=pl.ANY)
    dx_out = pl.BlockSpec((None, ROWS, D), lambda i: (i, 0, 0))
    dg_out = pl.BlockSpec((None, ROWS, 128), lambda i: (i, 0, 0))
    outs = [jax.ShapeDtypeStruct((CHUNK, ROWS, D), BF16), jax.ShapeDtypeStruct((CHUNK, ROWS, 128), F32)]
    out_specs = [dx_out, dg_out]
    if add_into:
        outs += [jax.ShapeDtypeStruct((CHUNK, HALF, WIDE), F32)] * 2
        out_specs += [anywhere, anywhere]
    else:
        outs += [jax.ShapeDtypeStruct((CHUNK, D, WIDE), F32)]
        out_specs += [anywhere]
    operands = [place, *rows, *pieces] + ([acc] if add_into else [])
    return pl.pallas_call(
        functools.partial(expert_kernel, add_into),
        grid=(CHUNK,),
        out_shape=tuple(outs),
        in_specs=[pl.BlockSpec(memory_space=pltpu.SMEM)] + [row_in] * 3 + [anywhere] * (4 + add_into),
        out_specs=tuple(out_specs),
        scratch_shapes=[
            pltpu.VMEM((CHUNK, D, WIDE), BF16),
            pltpu.VMEM((ROWS, F), BF16),
            pltpu.VMEM((ROWS, 2 * F), BF16),
            pltpu.VMEM((D, ROWS), BF16),
            pltpu.VMEM((D, ROWS), BF16),
            pltpu.VMEM((D, WIDE), F32),
            pltpu.SemaphoreType.DMA((CHUNK,)),
            pltpu.SemaphoreType.DMA,
            pltpu.SemaphoreType.DMA((2,)),
        ],
        compiler_params=params(),
        name="experts_second" if add_into else "experts_first",
        cost_estimate=pl.CostEstimate(flops=CHUNK * 18 * ROWS * D * F, bytes_accessed=CHUNK * (24 << 20), transcendentals=CHUNK * 2 * ROWS * F),
    )(*operands)


def combine_kernel(first_ref, *refs):
    dx_refs = refs[:N_CHUNK]
    dg_refs = refs[N_CHUNK:2 * N_CHUNK]
    pos_ref, ids_ref, out_ref, pick, rows = refs[2 * N_CHUNK:]
    first = first_ref[0]
    slots = lax.broadcasted_iota(jnp.int32, (CAP, TOK), 0)
    ids = ids_ref[...]
    dg_choice = jnp.zeros((TOP_K, TOK), F32)
    for e in range(EXP):
        k, j = divmod(e, CHUNK)
        hit = slots == pos_ref[e:e + 1, :]
        pick[e * CAP:(e + 1) * CAP, :] = jnp.where(hit, 1.0, 0.0).astype(BF16)
        dg_tok = jnp.sum(jnp.where(hit, dg_refs[k][j, :, :1], 0.0), axis=0, keepdims=True)
        dg_choice = dg_choice + jnp.where(ids == first + e, dg_tok, 0.0)
        rows[e * CAP:(e + 1) * CAP, :] = dx_refs[k][j]
    out_ref[:TOK, :] = lax.dot_general(pick[...], rows[...], (((0,), (0,)), ((), ())), preferred_element_type=F32)
    out_ref[TOK:TOK + 8, :] = dg_choice[:, :D]
    out_ref[TOK + 8:, :] = jnp.zeros((8, D), F32)
    out_ref[TOK + 8:, :TOK - D] = dg_choice[:, D:]


def combine(first, dx_rows, dg_rows, pos, ids, mb):
    dx_in = pl.BlockSpec((CHUNK, CAP, D), lambda s: (0, s, 0))
    dg_in = pl.BlockSpec((CHUNK, CAP, 128), lambda s: (0, s, 0))
    return pl.pallas_call(
        combine_kernel,
        grid=(SRC,),
        out_shape=jax.ShapeDtypeStruct((SRC, TOKEN_ROWS, D), F32),
        in_specs=[pl.BlockSpec(memory_space=pltpu.SMEM)] + [dx_in] * N_CHUNK + [dg_in] * N_CHUNK
        + [pl.BlockSpec((None, None, EXP, TOK), lambda s: (mb, s, 0, 0)), pl.BlockSpec((None, None, TOP_K, TOK), lambda s: (s, mb, 0, 0))],
        out_specs=pl.BlockSpec((None, TOKEN_ROWS, D), lambda s: (s, 0, 0)),
        scratch_shapes=[pltpu.VMEM((ROWS, TOK), BF16), pltpu.VMEM((ROWS, D), BF16)],
        compiler_params=params(),
        name="combine",
        cost_estimate=pl.CostEstimate(flops=2 * SRC * ROWS * TOK * D, bytes_accessed=60 << 20, transcendentals=0),
    )(first, *dx_rows, *dg_rows, pos, ids)


SWAP = [(0, 1), (1, 0)]
GROUP = ('y', 'x', 'c')


def solution(mesh):
    cube = Mesh(mesh.devices.reshape(2, 2, 2, 2), ('z', 'y', 'x', 'c'))
    tok_spec = P(None, ('z', 'y', 'x', 'c'), None)
    spec_edf = P(('x', 'c'), ('z', 'y'), None)
    spec_efd = P(('x', 'c'), None, ('z', 'y'))

    def local_step(x_in, dy_out, expert_idx, gate_prob, w_one, w_two, w_three):
        z, y, x, c = (lax.axis_index(name) for name in 'zyxc')
        place = jnp.stack([z, y]).astype(jnp.int32)
        first = ((x * 2 + c) * 16 + y * EXP).astype(jnp.int32).reshape(1)

        ids = lax.all_gather(jnp.swapaxes(expert_idx, 1, 2), GROUP, axis=0, tiled=False)
        gate = lax.all_gather(jnp.swapaxes(gate_prob, 1, 2), GROUP, axis=0, tiled=False)
        tokens = [
            lax.all_gather(jnp.concatenate([x_in[mb], dy_out[mb]], axis=0), GROUP, axis=0, tiled=False) for mb in range(MICRO)
        ]

        wide = jnp.concatenate([w_one, w_three, jnp.swapaxes(w_two, 1, 2)], axis=2)
        pieces = []
        for k in range(N_CHUNK):
            own = lax.dynamic_slice_in_dim(wide, y * EXP + k * CHUNK, CHUNK, 0)
            other = lax.dynamic_slice_in_dim(wide, (1 - y) * EXP + k * CHUNK, CHUNK, 0)
            from_y = lax.ppermute(other, 'y', SWAP)
            from_z = lax.ppermute(own, 'z', SWAP)
            from_yz = lax.ppermute(from_y, 'z', SWAP)
            pieces.append((own, from_y, from_z, from_yz))

        pos, gate_sel = routing(first, ids, gate)

        back = []
        acc = [None] * N_CHUNK
        for mb in range(MICRO):
            rows = gather_rows(tokens[mb], pos, gate_sel, mb)
            dx_rows, dg_rows = [], []
            for k in range(N_CHUNK):
                res = run_experts(place, rows, pieces[k], acc[k], k)
                dx_rows.append(res[0])
                dg_rows.append(res[1])
                acc[k] = res[2] if mb == 0 else res[2:]
            sums = combine(first, dx_rows, dg_rows, pos, ids, mb)
            back.append(lax.psum_scatter(sums, GROUP, scatter_dimension=0, tiled=True)[0])

        mine, theirs = [], []
        for k in range(N_CHUNK):
            keep, send = acc[k]
            total = keep + lax.ppermute(send, 'z', SWAP)
            mine.append(lax.dynamic_slice_in_dim(total, y * QUARTER, QUARTER, 1))
            out = lax.dynamic_slice_in_dim(total, (1 - y) * QUARTER, QUARTER, 1)
            theirs.append(lax.ppermute(out, 'y', SWAP))
        grads = []
        for part in range(3):
            cols = slice(part * F, (part + 1) * F)
            buf = jnp.zeros((2 * EXP, QUARTER, F), F32)
            for k in range(N_CHUNK):
                buf = lax.dynamic_update_slice_in_dim(buf, mine[k][:, :, cols], y * EXP + k * CHUNK, 0)
                buf = lax.dynamic_update_slice_in_dim(buf, theirs[k][:, :, cols], (1 - y) * EXP + k * CHUNK, 0)
            grads.append(buf)

        dx_in = jnp.stack([b[:TOK].astype(BF16) for b in back])
        d_gate = jnp.stack([jnp.concatenate([b[TOK:TOK + 8, :], b[TOK + 8:, :TOK - D]], axis=1) for b in back])
        return dx_in, jnp.swapaxes(d_gate, 1, 2), grads[0], jnp.swapaxes(grads[2], 1, 2), grads[1]

    return jax.shard_map(
        local_step,
        mesh=cube,
        in_specs=(tok_spec, tok_spec, tok_spec, tok_spec, spec_edf, spec_efd, spec_edf),
        out_specs=(tok_spec, tok_spec, spec_edf, spec_efd, spec_edf),
        check_vma=False,
    )
```

```python
import functools

import jax
import jax.numpy as jnp
from jax import lax
from jax.experimental import pallas as pl
from jax.experimental.pallas import tpu as pltpu
from jax.sharding import Mesh, PartitionSpec as P


MICRO = 2
TOK = 1024
TOP_K = 8
D = 896
F = 640
CAP = 160
SRC = 8
EXP = 8
QUARTER = D // 4
HALF = D // 2
ROWS = SRC * CAP
CHUNKS = (1, 2, 2, 2, 1)
STARTS = (0, 1, 3, 5, 7)
GRAIN = 16
TILE = 256
N_CHUNK = len(CHUNKS)
WIDE = 3 * F
SUM_ROWS = TOK + 16
TABLE_ROWS = 64

BF16 = jnp.bfloat16
F32 = jnp.float32
VMEM_LIMIT = 62 * 1024 * 1024


def params(**kw):
    return pltpu.CompilerParams(vmem_limit_bytes=VMEM_LIMIT, **kw)


PIECES = 4


def token_kernel(mb, x_ref, dy_ref, ids_ref, gate_ref, out_ref, buf, table, in_sem, out_sem):
    rows = TOK // PIECES
    loads = []
    for half, src in enumerate((x_ref, dy_ref)):
        for i in range(PIECES):
            place = pl.ds((half * PIECES + i) * rows, rows)
            loads.append(pltpu.make_async_copy(src.at[mb, pl.ds(i * rows, rows), :], buf.at[place, :], in_sem.at[half * PIECES + i]))
    for load in loads:
        load.start()
    gate = gate_ref[mb]
    high = gate.astype(BF16).astype(F32)
    mid = (gate - high).astype(BF16).astype(F32)
    low = gate - high - mid
    rows_f = jnp.concatenate([ids_ref[mb].astype(F32), high, mid, low], axis=0)
    table[:32, :] = rows_f[:, :D].astype(BF16)
    table[32:, :] = jnp.zeros((32, D), BF16)
    table[32:, :TOK - D] = rows_f[:, D:].astype(BF16)
    stores = []
    for i, load in enumerate(loads):
        load.wait()
        place = pl.ds(i * rows, rows)
        stores.append(pltpu.make_async_copy(buf.at[place, :], out_ref.at[place, :], out_sem))
        stores[-1].start()
    stores.append(pltpu.make_async_copy(table, out_ref.at[pl.ds(2 * TOK, TABLE_ROWS), :], out_sem))
    stores[-1].start()
    for store in stores:
        store.wait()


def token_block(x_in, dy_out, ids, gate, mb):
    anywhere = pl.BlockSpec(memory_space=pl.ANY)
    return pl.pallas_call(
        functools.partial(token_kernel, mb),
        out_shape=jax.ShapeDtypeStruct((2 * TOK + TABLE_ROWS, D), BF16),
        in_specs=[anywhere, anywhere, pl.BlockSpec(memory_space=pltpu.VMEM), pl.BlockSpec(memory_space=pltpu.VMEM)],
        out_specs=anywhere,
        scratch_shapes=[
            pltpu.VMEM((2 * TOK, D), BF16),
            pltpu.VMEM((TABLE_ROWS, D), BF16),
            pltpu.SemaphoreType.DMA((2 * PIECES,)),
            pltpu.SemaphoreType.DMA,
        ],
        compiler_params=params(),
        name="token_block",
        cost_estimate=pl.CostEstimate(flops=1 << 20, bytes_accessed=8 << 20, transcendentals=0),
    )(x_in, dy_out, ids, gate)


def routing_kernel(first_ref, *refs):
    tables = refs[:SRC]
    pos_ref, gsel_ref, ids_ref, cnt_ref, member = refs[SRC:]
    first = first_ref[0]
    for src in range(SRC):
        block = tables[src][...].astype(F32)
        table = jnp.concatenate([block[:32], block[32:, :TOK - D]], axis=1)
        ids = table[:8].astype(jnp.int32)
        gate = table[8:16] + table[16:24] + table[24:]
        ids_ref[src] = ids
        for e in range(EXP):
            hit = ids == first + e
            row = src * EXP + e
            member[row:row + 1, :] = jnp.sum(jnp.where(hit, 1.0, 0.0), axis=0, keepdims=True)
            gsel_ref[src, e:e + 1, :] = jnp.sum(jnp.where(hit, gate, 0.0), axis=0, keepdims=True)
    earlier = lax.broadcasted_iota(jnp.int32, (TOK, TOK), 0) < lax.broadcasted_iota(jnp.int32, (TOK, TOK), 1)
    chosen = member[...]
    count = jnp.dot(chosen.astype(BF16), jnp.where(earlier, 1.0, 0.0).astype(BF16), preferred_element_type=F32)
    kept = (chosen > 0.5) & (count < CAP - 0.5)
    slot = jnp.where(kept, count, -1.0).astype(jnp.int32)
    pos_ref[...] = slot.reshape(SRC, EXP, TOK)
    load = lax.dot_general(jnp.ones((8, TOK), BF16), chosen.astype(BF16), (((1,), (1,)), ((), ())), preferred_element_type=F32)
    rows = jnp.minimum(load, float(CAP)).astype(jnp.int32)
    cnt_ref[...] = ((rows + (GRAIN - 1)) >> 4) << 4


def routing(first, tokens):
    shape = (SRC, EXP, TOK)
    table = pl.BlockSpec((TABLE_ROWS, D), lambda i: (2 * TOK // TABLE_ROWS, 0))
    whole = pl.BlockSpec(shape, lambda i: (0, 0, 0))
    return pl.pallas_call(
        routing_kernel,
        grid=(1,),
        out_shape=(jax.ShapeDtypeStruct(shape, jnp.int32), jax.ShapeDtypeStruct(shape, F32), jax.ShapeDtypeStruct(shape, jnp.int32), jax.ShapeDtypeStruct((8, SRC * EXP), jnp.int32)),
        in_specs=[pl.BlockSpec(memory_space=pltpu.SMEM)] + [table] * SRC,
        out_specs=(whole, whole, whole, pl.BlockSpec((8, SRC * EXP), lambda i: (0, 0))),
        scratch_shapes=[pltpu.VMEM((SRC * EXP, TOK), F32)],
        compiler_params=params(),
        name="routing",
        cost_estimate=pl.CostEstimate(flops=2 * 64 * TOK * TOK, bytes_accessed=3 << 20, transcendentals=0),
    )(first, *tokens)


def aligned(value):
    return pl.multiple_of(value, GRAIN)


def gather_kernel(lo, n, cnt_ref, *refs):
    tok_refs = refs[:SRC]
    pos_ref, gate_ref = refs[SRC:SRC + 2]
    out_refs = refs[SRC + 2:SRC + 5]
    pick, gcol, buf, stage, offset, sem, out_sem = refs[SRC + 5:]
    s = pl.program_id(0)
    slot = lax.rem(s, 2)

    def fetch(src):
        return pltpu.make_async_copy(tok_refs[src].at[pl.ds(0, 2 * TOK), :], buf.at[src % 2], sem.at[src % 2])

    def store(which, j, side, start, place):
        return pltpu.make_async_copy(
            stage.at[side, which, pl.ds(aligned(start), CAP), :], out_refs[which].at[j, pl.ds(aligned(place), CAP), :], out_sem.at[side]
        )

    @pl.when(s == 0)
    def _():
        fetch(0).start()
        for j in range(n):
            offset[j] = 0

    for src in range(1, SRC):
        @pl.when(s == src - 1)
        def _(src=src):
            fetch(src).start()

    slots = lax.broadcasted_iota(jnp.int32, (CAP, TOK), 0)
    starts = []
    total = jnp.int32(0)
    for j in range(n):
        e = lo + j
        rows = pl.ds(aligned(total), CAP)
        hit = slots == pos_ref[e:e + 1, :]
        pick[rows, :] = jnp.where(hit, 1.0, 0.0).astype(BF16)
        col = jnp.sum(jnp.where(hit, gate_ref[e:e + 1, :], 0.0), axis=1, keepdims=True)
        gcol[rows, :] = jnp.broadcast_to(col, (CAP, 128))
        starts.append(total)
        total = total + cnt_ref[0, s * EXP + e]

    for src in range(SRC):
        @pl.when(s == src)
        def _(src=src):
            fetch(src).wait()

    def body(t, carry):
        rows = pl.ds(pl.multiple_of(t * TILE, TILE), TILE)
        sel = pick[rows, :]
        x_rows = jnp.dot(sel, buf[slot, :TOK, :], preferred_element_type=F32)
        stage[slot, 0, rows, :] = x_rows.astype(BF16)
        dy_rows = jnp.dot(sel, buf[slot, TOK:, :], preferred_element_type=F32)
        stage[slot, 1, rows, :] = dy_rows.astype(BF16)
        stage[slot, 2, rows, :] = (gcol[rows, :1] * dy_rows).astype(BF16)
        return carry

    lax.fori_loop(0, (total + (TILE - 1)) // TILE, body, 0)

    @pl.when(s > 0)
    def _():
        for j in range(n):
            for which in range(3):
                store(which, j, 1 - slot, 0, 0).wait()

    for j in range(n):
        place = offset[j]
        for which in range(3):
            store(which, j, slot, starts[j], place).start()
        offset[j] = place + cnt_ref[0, s * EXP + lo + j]

    @pl.when(s == SRC - 1)
    def _():
        for j in range(n):
            for which in range(3):
                store(which, j, slot, 0, 0).wait()


def gather_rows(counts, tokens, pos, gate, lo, n):
    rows = jax.ShapeDtypeStruct((n, ROWS, D), BF16)
    table = pl.BlockSpec((None, EXP, TOK), lambda s: (s, 0, 0))
    anywhere = pl.BlockSpec(memory_space=pl.ANY)
    picked = (n * CAP + TILE - 1) // TILE * TILE
    return pl.pallas_call(
        functools.partial(gather_kernel, lo, n),
        grid=(SRC,),
        out_shape=(rows, rows, rows),
        in_specs=[pl.BlockSpec(memory_space=pltpu.SMEM)] + [anywhere] * SRC + [table, table],
        out_specs=(anywhere, anywhere, anywhere),
        scratch_shapes=[
            pltpu.VMEM((picked, TOK), BF16),
            pltpu.VMEM((picked, 128), F32),
            pltpu.VMEM((2, 2 * TOK, D), BF16),
            pltpu.VMEM((2, 3, picked, D), BF16),
            pltpu.SMEM((n,), jnp.int32),
            pltpu.SemaphoreType.DMA((2,)),
            pltpu.SemaphoreType.DMA((2,)),
        ],
        compiler_params=params(),
        name="gather_rows",
        cost_estimate=pl.CostEstimate(flops=4 * SRC * n * CAP * TOK * D, bytes_accessed=(30 + 7 * n) << 20, transcendentals=0),
    )(counts, *tokens, pos, gate)


def expert_kernel(add_into, lo, n, place_ref, cnt_ref, x_ref, dy_ref, g_ref, own_ref, yr_ref, zo_ref, zf_ref, *refs):
    if add_into:
        acc_ref, dx_ref, dg_ref, keep_ref, send_ref = refs[:5]
        refs = refs[5:]
    else:
        dx_ref, dg_ref, part_ref = refs[:3]
        refs = refs[3:]
    w, dws, w_sem, acc_sem, out_sem = refs
    i = pl.program_id(0)
    side = lax.rem(i, 2)
    dw = dws.at[side]
    z, y = place_ref[0], place_ref[1]
    quarters = (2 * z + y, 2 * z + 1 - y, 2 * (1 - z) + y, 2 * (1 - z) + 1 - y)

    def weight_copies(j):
        return [
            pltpu.make_async_copy(ref.at[j], w.at[j, pl.ds(pl.multiple_of(q * QUARTER, QUARTER), QUARTER), :], w_sem.at[j])
            for ref, q in zip((own_ref, yr_ref, zo_ref, zf_ref), quarters)
        ]

    def acc_copy(j):
        return pltpu.make_async_copy(acc_ref.at[j], dws.at[lax.rem(j, 2)], acc_sem)

    def out_copies(j):
        total = dws.at[lax.rem(j, 2)]
        if not add_into:
            return [pltpu.make_async_copy(total, part_ref.at[j], out_sem.at[0])]
        return [
            pltpu.make_async_copy(total.at[pl.ds(pl.multiple_of(z * HALF, HALF), HALF), :], keep_ref.at[j], out_sem.at[0]),
            pltpu.make_async_copy(total.at[pl.ds(pl.multiple_of((1 - z) * HALF, HALF), HALF), :], send_ref.at[j], out_sem.at[1]),
        ]

    @pl.when(i == 0)
    def _():
        for j in range(n):
            for copy in weight_copies(j):
                copy.start()
        if add_into:
            acc_copy(0).start()

    count = cnt_ref[0, lo + i]
    for src in range(1, SRC):
        count = count + cnt_ref[0, src * EXP + lo + i]

    if not add_into:
        dw[...] = jnp.zeros((D, WIDE), F32)
    for copy in weight_copies(i):
        copy.wait()
    if add_into:
        acc_copy(i).wait()

    def tile(start, size):
        rows = pl.ds(pl.multiple_of(start, TILE), size)
        live = lax.broadcasted_iota(jnp.int32, (size, 1), 0) < count - start
        x_c = jnp.where(live, x_ref[rows, :].astype(F32), 0.0).astype(BF16)
        g_c = jnp.where(live, g_ref[rows, :].astype(F32), 0.0).astype(BF16)
        h = jnp.dot(x_c, w[i, :, :2 * F], preferred_element_type=F32)
        h_one = h[:, :F]
        h_three = h[:, F:]
        sigma = jax.nn.sigmoid(h_one)
        silu = h_one * sigma
        act = (silu * h_three).astype(BF16)
        back = jnp.dot(dy_ref[rows, :], w[i, :, 2 * F:], preferred_element_type=F32)
        dg = jnp.sum(act.astype(F32) * back, axis=1, keepdims=True)
        dg_ref[rows, :] = jnp.broadcast_to(dg, (size, 128))
        d_act = jnp.dot(g_c, w[i, :, 2 * F:], preferred_element_type=F32)
        dh_three = (d_act * silu).astype(BF16)
        dh_one = (d_act * h_three * sigma * (1.0 + h_one * (1.0 - sigma))).astype(BF16)
        dh = jnp.concatenate([dh_one, dh_three], axis=1)
        dx = lax.dot_general(dh, w[i, :, :2 * F], (((1,), (1,)), ((), ())), preferred_element_type=F32)
        dx_ref[rows, :] = dx.astype(BF16)
        dw[:, :2 * F] += jnp.dot(x_c.T, dh, preferred_element_type=F32)
        dw[:, 2 * F:] += jnp.dot(g_c.T, act, preferred_element_type=F32)

    pairs = (count + (TILE - 1)) // (2 * TILE)

    def body(t, carry):
        tile(t * (2 * TILE), 2 * TILE)
        return carry

    lax.fori_loop(0, pairs, body, 0)

    @pl.when(pairs * (2 * TILE) < count)
    def _():
        tile(pairs * (2 * TILE), TILE)

    @pl.when(i > 0)
    def _():
        for copy in out_copies(i - 1):
            copy.wait()

    for copy in out_copies(i):
        copy.start()
    if add_into:
        @pl.when(i + 1 < n)
        def _():
            acc_copy(i + 1).start()

    @pl.when(i == n - 1)
    def _():
        for copy in out_copies(i):
            copy.wait()


def run_experts(place, counts, rows, offset, pieces, acc, k):
    add_into = acc is not None
    n = CHUNKS[k]
    row_in = pl.BlockSpec((None, ROWS, D), lambda i: (offset + i, 0, 0))
    anywhere = pl.BlockSpec(memory_space=pl.ANY)
    dx_out = pl.BlockSpec((None, ROWS, D), lambda i: (i, 0, 0))
    dg_out = pl.BlockSpec((None, ROWS, 128), lambda i: (i, 0, 0))
    outs = [jax.ShapeDtypeStruct((n, ROWS, D), BF16), jax.ShapeDtypeStruct((n, ROWS, 128), F32)]
    out_specs = [dx_out, dg_out]
    if add_into:
        outs += [jax.ShapeDtypeStruct((n, HALF, WIDE), F32)] * 2
        out_specs += [anywhere, anywhere]
    else:
        outs += [jax.ShapeDtypeStruct((n, D, WIDE), F32)]
        out_specs += [anywhere]
    operands = [place, counts, *rows, *pieces] + ([acc] if add_into else [])
    smem = pl.BlockSpec(memory_space=pltpu.SMEM)
    return pl.pallas_call(
        functools.partial(expert_kernel, add_into, STARTS[k], n),
        grid=(n,),
        out_shape=tuple(outs),
        in_specs=[smem, smem] + [row_in] * 3 + [anywhere] * (4 + add_into),
        out_specs=tuple(out_specs),
        scratch_shapes=[
            pltpu.VMEM((n, D, WIDE), BF16),
            pltpu.VMEM((2, D, WIDE), F32),
            pltpu.SemaphoreType.DMA((n,)),
            pltpu.SemaphoreType.DMA,
            pltpu.SemaphoreType.DMA((2,)),
        ],
        compiler_params=params(),
        name="experts_second" if add_into else "experts_first",
        cost_estimate=pl.CostEstimate(flops=n * 18 * ROWS * D * F, bytes_accessed=n * (24 << 20), transcendentals=n * 2 * ROWS * F),
    )(*operands)


def combine_kernel(base, steps, extras, final, first_ref, cnt_ref, *refs):
    dx_refs = refs[:N_CHUNK]
    dg_refs = refs[N_CHUNK:2 * N_CHUNK]
    refs = refs[2 * N_CHUNK:]
    pos_ref, ids_ref = refs[:2]
    extra_refs = refs[2:2 + extras]
    refs = refs[2 + extras:]
    if final == 2:
        refs = refs[2:]
    if final:
        dx_out, dg_out, sums = refs[:3]
        refs = refs[3:]
    else:
        sums = refs[0]
        refs = refs[1:]
    pick, rows, stage, dg_stage, sem = refs
    step = pl.program_id(0)
    side = lax.rem(step, 2)
    first = first_ref[0]

    def loads(i):
        source = base + 2 * i
        out = []
        for k in range(N_CHUNK):
            for j in range(CHUNKS[k]):
                e = STARTS[k] + j
                place = jnp.int32(0)
                for src in range(SRC - 1):
                    place = place + jnp.where(src < source, cnt_ref[0, src * EXP + e], 0)
                window = pl.ds(aligned(place), CAP)
                out.append(pltpu.make_async_copy(dx_refs[k].at[j, window, :], stage.at[lax.rem(i, 2), e], sem.at[lax.rem(i, 2)]))
                out.append(pltpu.make_async_copy(dg_refs[k].at[j, window, :], dg_stage.at[lax.rem(i, 2), e], sem.at[lax.rem(i, 2)]))
        return out

    @pl.when(step == 0)
    def _():
        for load in loads(step):
            load.start()
        rows[...] = jnp.zeros((ROWS + TILE, D), BF16)

    @pl.when(step + 1 < steps)
    def _():
        for load in loads(step + 1):
            load.start()

    source = base + 2 * step
    slots = lax.broadcasted_iota(jnp.int32, (CAP, TOK), 0)
    total = jnp.int32(0)
    starts, counts = [], []
    for e in range(EXP):
        pick[pl.ds(aligned(total), CAP), :] = jnp.where(slots == pos_ref[e:e + 1, :], 1.0, 0.0).astype(BF16)
        starts.append(total)
        counts.append(cnt_ref[0, source * EXP + e])
        total = total + counts[e]
    pick[pl.ds(aligned(total), TILE), :] = jnp.zeros((TILE, TOK), BF16)

    for load in loads(step):
        load.wait()
    ids = ids_ref[...]
    dg_choice = jnp.zeros((TOP_K, TOK), F32)
    for e in range(EXP):
        block = stage[side, e]
        if e == EXP - 1:
            live = lax.broadcasted_iota(jnp.int32, (CAP, 1), 0) < counts[e]
            block = jnp.where(live, block.astype(F32), 0.0).astype(BF16)
        rows[pl.ds(aligned(starts[e]), CAP), :] = block
        hit = slots == pos_ref[e:e + 1, :]
        dg_tok = jnp.sum(jnp.where(hit, dg_stage[side, e, :, :1], 0.0), axis=0, keepdims=True)
        dg_choice = dg_choice + jnp.where(ids == first + e, dg_tok, 0.0)

    start = jnp.zeros((TOK, D), F32)
    left = dg_choice[:, :D]
    right = dg_choice[:, D:]
    for extra in extra_refs:
        start = start + extra[:TOK, :]
        left = left + extra[TOK:TOK + 8, :]
        right = right + extra[TOK + 8:, :TOK - D]
    sums[:TOK, :] = start

    def body(t, carry):
        part = pl.ds(pl.multiple_of(t * TILE, TILE), TILE)
        sums[:TOK, :] += lax.dot_general(pick[part, :], rows[part, :], (((0,), (0,)), ((), ())), preferred_element_type=F32)
        return carry

    lax.fori_loop(0, (total + (TILE - 1)) // TILE, body, 0)
    if final:
        dx_out[...] = sums[:TOK, :].astype(BF16)
        dg_out[:, :D] = left
        dg_out[:, D:] = right
    else:
        sums[TOK:TOK + 8, :] = left
        sums[TOK + 8:, :] = jnp.zeros((8, D), F32)
        sums[TOK + 8:, :TOK - D] = right


def combine(first, table, dx_rows, dg_rows, base, steps, partner=None, arrived=(), final=None, mb=0):
    pos, ids, counts = table
    smem = pl.BlockSpec(memory_space=pltpu.SMEM)
    anywhere = pl.BlockSpec(memory_space=pl.ANY)
    block = pl.BlockSpec((None, EXP, TOK), lambda i: (base + 2 * i, 0, 0))
    whole = pl.BlockSpec((SUM_ROWS, D), lambda i: (0, 0))
    extra_specs = [] if partner is None else [pl.BlockSpec((None, SUM_ROWS, D), lambda i: (base // 2, 0, 0))]
    extra_specs += [whole] * len(arrived)
    extra = ([] if partner is None else [partner]) + list(arrived)
    scratch = [
        pltpu.VMEM((ROWS + TILE, TOK), BF16),
        pltpu.VMEM((ROWS + TILE, D), BF16),
        pltpu.VMEM((2, EXP, CAP, D), BF16),
        pltpu.VMEM((2, EXP, CAP, 128), F32),
        pltpu.SemaphoreType.DMA((2,)),
    ]
    in_specs = [smem, smem] + [anywhere] * (2 * N_CHUNK) + [block, block] + extra_specs
    operands = [first, counts, *dx_rows, *dg_rows, pos, ids, *extra]
    mode, aliases = 0, {}
    if final is None:
        if steps > 1:
            outs = jax.ShapeDtypeStruct((steps, SUM_ROWS, D), F32)
            out_specs = pl.BlockSpec((None, SUM_ROWS, D), lambda i: (i, 0, 0))
        else:
            outs, out_specs = jax.ShapeDtypeStruct((SUM_ROWS, D), F32), whole
    else:
        outs = (jax.ShapeDtypeStruct((MICRO, TOK, D), BF16), jax.ShapeDtypeStruct((MICRO, TOP_K, TOK), F32))
        out_specs = (pl.BlockSpec((None, TOK, D), lambda i: (mb, 0, 0)), pl.BlockSpec((None, TOP_K, TOK), lambda i: (mb, 0, 0)))
        scratch = [pltpu.VMEM((TOK, D), F32)] + scratch
        mode = 1
        if final:
            mode = 2
            aliases = {len(operands): 0, len(operands) + 1: 1}
            in_specs += [anywhere, anywhere]
            operands += list(final)
    return pl.pallas_call(
        functools.partial(combine_kernel, base, steps, len(extra), mode),
        grid=(steps,),
        out_shape=outs,
        in_specs=in_specs,
        out_specs=out_specs,
        scratch_shapes=scratch,
        input_output_aliases=aliases,
        compiler_params=params(),
        name="combine",
        cost_estimate=pl.CostEstimate(flops=steps * 2 * ROWS * TOK * D, bytes_accessed=steps * (8 << 20), transcendentals=0),
    )(*operands)


SWAP = [(0, 1), (1, 0)]


def swap(value, axis):
    return lax.ppermute(value, axis, SWAP)


def solution(mesh):
    cube = Mesh(mesh.devices.reshape(2, 2, 2, 2), ('z', 'y', 'x', 'c'))
    tok_spec = P(None, ('z', 'y', 'x', 'c'), None)
    spec_edf = P(('x', 'c'), ('z', 'y'), None)
    spec_efd = P(('x', 'c'), None, ('z', 'y'))

    def gather_tokens(block):
        from_y = swap(block, 'y')
        from_x = swap(block, 'x')
        from_xy = swap(from_y, 'x')
        return [
            block, swap(block, 'c'),
            from_x, swap(from_x, 'c'),
            from_y, swap(from_y, 'c'),
            from_xy, swap(from_xy, 'c'),
        ]

    def local_step(x_in, dy_out, expert_idx, gate_prob, w_one, w_two, w_three):
        z, y, x, c = (lax.axis_index(name) for name in 'zyxc')
        place = jnp.stack([z, y]).astype(jnp.int32)
        first = ((x * 2 + c) * 16 + y * EXP).astype(jnp.int32).reshape(1)
        ids = jnp.swapaxes(expert_idx, 1, 2)
        gate = jnp.swapaxes(gate_prob, 1, 2)

        tokens = [gather_tokens(token_block(x_in, dy_out, ids, gate, mb)) for mb in range(MICRO)]

        w_two_t = jnp.swapaxes(w_two, 1, 2)

        def shard(half, k):
            cut = [lax.dynamic_slice_in_dim(w, half * EXP + STARTS[k], CHUNKS[k], 0) for w in (w_one, w_three, w_two_t)]
            return jnp.concatenate(cut, axis=2)

        pieces = []
        for k in range(N_CHUNK):
            own = shard(y, k)
            from_y = swap(shard(1 - y, k), 'y')
            from_z = swap(own, 'z')
            from_yz = swap(from_y, 'z')
            pieces.append((own, from_y, from_z, from_yz))

        tables = [routing(first, tokens[mb]) for mb in range(MICRO)]
        split = STARTS[2]

        def gather(mb, lo, n):
            pos, gate_sel, _, counts = tables[mb]
            return gather_rows(counts, tokens[mb], pos, gate_sel, lo, n)

        whole = gather(0, 0, EXP)
        head = gather(1, 0, split)
        tail = gather(1, split, EXP - split)

        acc, keep, send = [], [], []
        dx_rows, dg_rows = ([], []), ([], [])
        for k in range(N_CHUNK):
            res = run_experts(place, tables[0][3], whole, STARTS[k], pieces[k], None, k)
            dx_rows[0].append(res[0])
            dg_rows[0].append(res[1])
            acc.append(res[2])
        for k in range(N_CHUNK):
            rows, offset = (head, STARTS[k]) if STARTS[k] < split else (tail, STARTS[k] - split)
            res = run_experts(place, tables[1][3], rows, offset, pieces[k], acc[k], k)
            dx_rows[1].append(res[0])
            dg_rows[1].append(res[1])
            keep.append(res[2])
            send.append(res[3])

        done = ()
        for mb in range(MICRO):
            pos, _, id_table, counts = tables[mb]
            args = (first, (pos, id_table, counts), dx_rows[mb], dg_rows[mb])
            partner = swap(combine(*args, 1, 4), 'c')
            far = swap(combine(*args, 6, 1, partner), 'x')
            near = swap(combine(*args, 2, 1, partner), 'x')
            last = swap(combine(*args, 4, 1, partner, (far,)), 'y')
            done = combine(*args, 0, 1, partner, (near, last), final=done, mb=mb)

        bufs = [jnp.zeros((2 * EXP, QUARTER, F), F32)] * 3
        for k in range(N_CHUNK):
            other = swap(send[k], 'z')

            def cut(which):
                return lax.dynamic_slice_in_dim(keep[k], which * QUARTER, QUARTER, 1) + lax.dynamic_slice_in_dim(other, which * QUARTER, QUARTER, 1)

            theirs = swap(cut(1 - y), 'y')
            mine = cut(y)
            for part in range(3):
                cols = slice(part * F, (part + 1) * F)
                buf = lax.dynamic_update_slice_in_dim(bufs[part], mine[:, :, cols], y * EXP + STARTS[k], 0)
                bufs[part] = lax.dynamic_update_slice_in_dim(buf, theirs[:, :, cols], (1 - y) * EXP + STARTS[k], 0)

        dx_in, d_gate = done
        return dx_in, jnp.swapaxes(d_gate, 1, 2), bufs[0], jnp.swapaxes(bufs[2], 1, 2), bufs[1]

    return jax.shard_map(
        local_step,
        mesh=cube,
        in_specs=(tok_spec, tok_spec, tok_spec, tok_spec, spec_edf, spec_efd, spec_edf),
        out_specs=(tok_spec, tok_spec, spec_edf, spec_efd, spec_edf),
        check_vma=False,
    )
```

```python
import functools

import jax
import jax.numpy as jnp
from jax import lax
from jax.experimental import pallas as pl
from jax.experimental.pallas import tpu as pltpu
from jax.sharding import Mesh, PartitionSpec as P


MICRO = 2
TOK = 1024
TOP_K = 8
D = 896
F = 640
CAP = 160
SRC = 8
PAIRS = SRC // 2
EXP = 8
QUARTER = D // 4
HALF = D // 2
ROWS = SRC * CAP
CHUNKS = (1, 2, 2, 2, 1)
STARTS = (0, 1, 3, 5, 7)
GRAIN = 16
TILE = 256
N_CHUNK = len(CHUNKS)
WIDE = 3 * F
SUM_ROWS = TOK + 16
TABLE_ROWS = 64

BF16 = jnp.bfloat16
F32 = jnp.float32
VMEM_LIMIT = 62 * 1024 * 1024


def params(**kw):
    return pltpu.CompilerParams(vmem_limit_bytes=VMEM_LIMIT, **kw)


PIECES = 4


def token_kernel(mb, x_ref, dy_ref, ids_ref, gate_ref, out_ref, buf, table, in_sem, out_sem):
    rows = TOK // PIECES
    loads = []
    for half, src in enumerate((x_ref, dy_ref)):
        for i in range(PIECES):
            place = pl.ds((half * PIECES + i) * rows, rows)
            loads.append(pltpu.make_async_copy(src.at[mb, pl.ds(i * rows, rows), :], buf.at[place, :], in_sem.at[half * PIECES + i]))
    for load in loads:
        load.start()
    gate = gate_ref[mb]
    high = gate.astype(BF16).astype(F32)
    mid = (gate - high).astype(BF16).astype(F32)
    low = gate - high - mid
    rows_f = jnp.concatenate([ids_ref[mb].astype(F32), high, mid, low], axis=0)
    table[:32, :] = rows_f[:, :D].astype(BF16)
    table[32:, :] = jnp.zeros((32, D), BF16)
    table[32:, :TOK - D] = rows_f[:, D:].astype(BF16)
    stores = []
    for i, load in enumerate(loads):
        load.wait()
        place = pl.ds(i * rows, rows)
        stores.append(pltpu.make_async_copy(buf.at[place, :], out_ref.at[place, :], out_sem))
        stores[-1].start()
    stores.append(pltpu.make_async_copy(table, out_ref.at[pl.ds(2 * TOK, TABLE_ROWS), :], out_sem))
    stores[-1].start()
    for store in stores:
        store.wait()


def token_block(x_in, dy_out, ids, gate, mb):
    anywhere = pl.BlockSpec(memory_space=pl.ANY)
    return pl.pallas_call(
        functools.partial(token_kernel, mb),
        out_shape=jax.ShapeDtypeStruct((2 * TOK + TABLE_ROWS, D), BF16),
        in_specs=[anywhere, anywhere, pl.BlockSpec(memory_space=pltpu.VMEM), pl.BlockSpec(memory_space=pltpu.VMEM)],
        out_specs=anywhere,
        scratch_shapes=[
            pltpu.VMEM((2 * TOK, D), BF16),
            pltpu.VMEM((TABLE_ROWS, D), BF16),
            pltpu.SemaphoreType.DMA((2 * PIECES,)),
            pltpu.SemaphoreType.DMA,
        ],
        compiler_params=params(),
        name="token_block",
        cost_estimate=pl.CostEstimate(flops=1 << 20, bytes_accessed=8 << 20, transcendentals=0),
    )(x_in, dy_out, ids, gate)


def routing_kernel(first_ref, *refs):
    tables = refs[:2]
    pos_ref, gsel_ref, ids_ref, cnt_ref, member = refs[2:]
    first = first_ref[0]
    for src in range(2):
        block = tables[src][...].astype(F32)
        table = jnp.concatenate([block[:32], block[32:, :TOK - D]], axis=1)
        ids = table[:8].astype(jnp.int32)
        gate = table[8:16] + table[16:24] + table[24:]
        ids_ref[src] = ids
        for e in range(EXP):
            hit = ids == first + e
            row = src * EXP + e
            member[row:row + 1, :] = jnp.sum(jnp.where(hit, 1.0, 0.0), axis=0, keepdims=True)
            gsel_ref[src, e:e + 1, :] = jnp.sum(jnp.where(hit, gate, 0.0), axis=0, keepdims=True)
    earlier = lax.broadcasted_iota(jnp.int32, (TOK, TOK), 0) < lax.broadcasted_iota(jnp.int32, (TOK, TOK), 1)
    chosen = member[...]
    count = jnp.dot(chosen.astype(BF16), jnp.where(earlier, 1.0, 0.0).astype(BF16), preferred_element_type=F32)
    kept = (chosen > 0.5) & (count < CAP - 0.5)
    slot = jnp.where(kept, count, -1.0).astype(jnp.int32)
    pos_ref[...] = slot.reshape(2, EXP, TOK)
    load = lax.dot_general(jnp.ones((8, TOK), BF16), chosen.astype(BF16), (((1,), (1,)), ((), ())), preferred_element_type=F32)
    rows = jnp.minimum(load, float(CAP)).astype(jnp.int32)
    cnt_ref[...] = ((rows + (GRAIN - 1)) >> 4) << 4


def routing(first, tokens):
    shape = (2, EXP, TOK)
    table = pl.BlockSpec((TABLE_ROWS, D), lambda i: (2 * TOK // TABLE_ROWS, 0))
    whole = pl.BlockSpec(shape, lambda i: (0, 0, 0))
    return pl.pallas_call(
        routing_kernel,
        grid=(1,),
        out_shape=(jax.ShapeDtypeStruct(shape, jnp.int32), jax.ShapeDtypeStruct(shape, F32), jax.ShapeDtypeStruct(shape, jnp.int32), jax.ShapeDtypeStruct((8, 2 * EXP), jnp.int32)),
        in_specs=[pl.BlockSpec(memory_space=pltpu.SMEM)] + [table] * 2,
        out_specs=(whole, whole, whole, pl.BlockSpec((8, 2 * EXP), lambda i: (0, 0))),
        scratch_shapes=[pltpu.VMEM((2 * EXP, TOK), F32)],
        compiler_params=params(),
        name="routing",
        cost_estimate=pl.CostEstimate(flops=2 * 16 * TOK * TOK, bytes_accessed=1 << 20, transcendentals=0),
    )(first, *tokens)


def count_at(cnt_refs, src, e):
    return cnt_refs[src // 2][0, (src % 2) * EXP + e]


def aligned(value):
    return pl.multiple_of(value, GRAIN)


def gather_kernel(pair, *refs):
    cnt_refs = refs[:pair + 1]
    refs = refs[pair + 1:]
    tok_refs = refs[:2]
    pos_ref, gate_ref = refs[2:4]
    refs = refs[4 + (3 if pair else 0):]
    out_refs = refs[:3]
    pick, gcol, buf, stage, offset, sem, out_sem = refs[3:]
    s = pl.program_id(0)

    def fetch(src):
        return pltpu.make_async_copy(tok_refs[src].at[pl.ds(0, 2 * TOK), :], buf.at[src], sem.at[src])

    def store(which, e, side, start, place):
        return pltpu.make_async_copy(
            stage.at[side, which, pl.ds(aligned(start), CAP), :], out_refs[which].at[e, pl.ds(aligned(place), CAP), :], out_sem.at[side]
        )

    @pl.when(s == 0)
    def _():
        fetch(0).start()
        fetch(1).start()
        for e in range(EXP):
            place = jnp.int32(0)
            for src in range(2 * pair):
                place = place + count_at(cnt_refs, src, e)
            offset[e] = place

    slots = lax.broadcasted_iota(jnp.int32, (CAP, TOK), 0)
    starts = []
    total = jnp.int32(0)
    for e in range(EXP):
        rows = pl.ds(aligned(total), CAP)
        hit = slots == pos_ref[e:e + 1, :]
        pick[rows, :] = jnp.where(hit, 1.0, 0.0).astype(BF16)
        col = jnp.sum(jnp.where(hit, gate_ref[e:e + 1, :], 0.0), axis=1, keepdims=True)
        gcol[rows, :] = jnp.broadcast_to(col, (CAP, 128))
        starts.append(total)
        total = total + cnt_refs[pair][0, s * EXP + e]

    for src in range(2):
        @pl.when(s == src)
        def _(src=src):
            fetch(src).wait()

    def body(t, carry):
        rows = pl.ds(pl.multiple_of(t * TILE, TILE), TILE)
        sel = pick[rows, :]
        x_rows = jnp.dot(sel, buf[s, :TOK, :], preferred_element_type=F32)
        stage[s, 0, rows, :] = x_rows.astype(BF16)
        dy_rows = jnp.dot(sel, buf[s, TOK:, :], preferred_element_type=F32)
        stage[s, 1, rows, :] = dy_rows.astype(BF16)
        stage[s, 2, rows, :] = (gcol[rows, :1] * dy_rows).astype(BF16)
        return carry

    lax.fori_loop(0, (total + (TILE - 1)) // TILE, body, 0)

    @pl.when(s > 0)
    def _():
        for e in range(EXP):
            for which in range(3):
                store(which, e, 0, 0, 0).wait()

    for e in range(EXP):
        place = offset[e]
        for which in range(3):
            store(which, e, s, starts[e], place).start()
        offset[e] = place + cnt_refs[pair][0, s * EXP + e]

    @pl.when(s == 1)
    def _():
        for e in range(EXP):
            for which in range(3):
                store(which, e, 1, 0, 0).wait()


def gather_rows(tables, tokens, rows, pair):
    shape = jax.ShapeDtypeStruct((EXP, ROWS, D), BF16)
    pos, gate = tables[pair][:2]
    counts = [table[3] for table in tables[:pair + 1]]
    table = pl.BlockSpec((None, EXP, TOK), lambda s: (s, 0, 0))
    anywhere = pl.BlockSpec(memory_space=pl.ANY)
    given = [] if rows is None else list(rows)
    operands = [*counts, *tokens[2 * pair:2 * pair + 2], pos, gate, *given]
    return pl.pallas_call(
        functools.partial(gather_kernel, pair),
        grid=(2,),
        out_shape=(shape, shape, shape),
        in_specs=[pl.BlockSpec(memory_space=pltpu.SMEM)] * (pair + 1) + [anywhere] * 2 + [table, table] + [anywhere] * len(given),
        out_specs=(anywhere, anywhere, anywhere),
        input_output_aliases={len(operands) - 3 + i: i for i in range(3)} if given else {},
        scratch_shapes=[
            pltpu.VMEM((ROWS, TOK), BF16),
            pltpu.VMEM((ROWS, 128), F32),
            pltpu.VMEM((2, 2 * TOK, D), BF16),
            pltpu.VMEM((2, 3, ROWS, D), BF16),
            pltpu.SMEM((EXP,), jnp.int32),
            pltpu.SemaphoreType.DMA((2,)),
            pltpu.SemaphoreType.DMA((2,)),
        ],
        compiler_params=params(),
        name="gather_rows",
        cost_estimate=pl.CostEstimate(flops=8 * ROWS * TOK * D, bytes_accessed=20 << 20, transcendentals=0),
    )(*operands)


def expert_kernel(add_into, lo, n, place_ref, *refs):
    cnt_refs = refs[:PAIRS]
    x_ref, dy_ref, g_ref, own_ref, yr_ref, zo_ref, zf_ref = refs[PAIRS:PAIRS + 7]
    refs = refs[PAIRS + 7:]
    if add_into:
        acc_ref, dx_ref, dg_ref, keep_ref, send_ref = refs[:5]
        refs = refs[5:]
    else:
        dx_ref, dg_ref, part_ref = refs[:3]
        refs = refs[3:]
    w, dws, w_sem, acc_sem, out_sem = refs
    i = pl.program_id(0)
    side = lax.rem(i, 2)
    dw = dws.at[side]
    z, y = place_ref[0], place_ref[1]
    quarters = (2 * z + y, 2 * z + 1 - y, 2 * (1 - z) + y, 2 * (1 - z) + 1 - y)

    def weight_copies(j):
        return [
            pltpu.make_async_copy(ref.at[j], w.at[j, pl.ds(pl.multiple_of(q * QUARTER, QUARTER), QUARTER), :], w_sem.at[j])
            for ref, q in zip((own_ref, yr_ref, zo_ref, zf_ref), quarters)
        ]

    def acc_copy(j):
        return pltpu.make_async_copy(acc_ref.at[j], dws.at[lax.rem(j, 2)], acc_sem)

    def out_copies(j):
        total = dws.at[lax.rem(j, 2)]
        if not add_into:
            return [pltpu.make_async_copy(total, part_ref.at[j], out_sem.at[0])]
        return [
            pltpu.make_async_copy(total.at[pl.ds(pl.multiple_of(z * HALF, HALF), HALF), :], keep_ref.at[j], out_sem.at[0]),
            pltpu.make_async_copy(total.at[pl.ds(pl.multiple_of((1 - z) * HALF, HALF), HALF), :], send_ref.at[j], out_sem.at[1]),
        ]

    @pl.when(i == 0)
    def _():
        for j in range(n):
            for copy in weight_copies(j):
                copy.start()
        if add_into:
            acc_copy(0).start()

    count = count_at(cnt_refs, 0, lo + i)
    for src in range(1, SRC):
        count = count + count_at(cnt_refs, src, lo + i)

    if not add_into:
        dw[...] = jnp.zeros((D, WIDE), F32)
    for copy in weight_copies(i):
        copy.wait()
    if add_into:
        acc_copy(i).wait()

    def tile(start, size):
        rows = pl.ds(pl.multiple_of(start, TILE), size)
        live = lax.broadcasted_iota(jnp.int32, (size, 1), 0) < count - start
        x_c = jnp.where(live, x_ref[rows, :].astype(F32), 0.0).astype(BF16)
        g_c = jnp.where(live, g_ref[rows, :].astype(F32), 0.0).astype(BF16)
        h = jnp.dot(x_c, w[i, :, :2 * F], preferred_element_type=F32)
        h_one = h[:, :F]
        h_three = h[:, F:]
        sigma = jax.nn.sigmoid(h_one)
        silu = h_one * sigma
        act = (silu * h_three).astype(BF16)
        back = jnp.dot(dy_ref[rows, :], w[i, :, 2 * F:], preferred_element_type=F32)
        dg = jnp.sum(act.astype(F32) * back, axis=1, keepdims=True)
        dg_ref[rows, :] = jnp.broadcast_to(dg, (size, 128))
        d_act = jnp.dot(g_c, w[i, :, 2 * F:], preferred_element_type=F32)
        dh_three = (d_act * silu).astype(BF16)
        dh_one = (d_act * h_three * sigma * (1.0 + h_one * (1.0 - sigma))).astype(BF16)
        dh = jnp.concatenate([dh_one, dh_three], axis=1)
        dx = lax.dot_general(dh, w[i, :, :2 * F], (((1,), (1,)), ((), ())), preferred_element_type=F32)
        dx_ref[rows, :] = dx.astype(BF16)
        dw[:, :2 * F] += jnp.dot(x_c.T, dh, preferred_element_type=F32)
        dw[:, 2 * F:] += jnp.dot(g_c.T, act, preferred_element_type=F32)

    pairs = (count + (TILE - 1)) // (2 * TILE)

    def body(t, carry):
        tile(t * (2 * TILE), 2 * TILE)
        return carry

    lax.fori_loop(0, pairs, body, 0)

    @pl.when(pairs * (2 * TILE) < count)
    def _():
        tile(pairs * (2 * TILE), TILE)

    @pl.when(i > 0)
    def _():
        for copy in out_copies(i - 1):
            copy.wait()

    for copy in out_copies(i):
        copy.start()
    if add_into:
        @pl.when(i + 1 < n)
        def _():
            acc_copy(i + 1).start()

    @pl.when(i == n - 1)
    def _():
        for copy in out_copies(i):
            copy.wait()


def run_experts(place, counts, rows, pieces, acc, k):
    add_into = acc is not None
    n = CHUNKS[k]
    row_in = pl.BlockSpec((None, ROWS, D), lambda i: (STARTS[k] + i, 0, 0))
    anywhere = pl.BlockSpec(memory_space=pl.ANY)
    dx_out = pl.BlockSpec((None, ROWS, D), lambda i: (i, 0, 0))
    dg_out = pl.BlockSpec((None, ROWS, 128), lambda i: (i, 0, 0))
    outs = [jax.ShapeDtypeStruct((n, ROWS, D), BF16), jax.ShapeDtypeStruct((n, ROWS, 128), F32)]
    out_specs = [dx_out, dg_out]
    if add_into:
        outs += [jax.ShapeDtypeStruct((n, HALF, WIDE), F32)] * 2
        out_specs += [anywhere, anywhere]
    else:
        outs += [jax.ShapeDtypeStruct((n, D, WIDE), F32)]
        out_specs += [anywhere]
    operands = [place, *counts, *rows, *pieces] + ([acc] if add_into else [])
    smem = pl.BlockSpec(memory_space=pltpu.SMEM)
    return pl.pallas_call(
        functools.partial(expert_kernel, add_into, STARTS[k], n),
        grid=(n,),
        out_shape=tuple(outs),
        in_specs=[smem] * (1 + PAIRS) + [row_in] * 3 + [anywhere] * (4 + add_into),
        out_specs=tuple(out_specs),
        scratch_shapes=[
            pltpu.VMEM((n, D, WIDE), BF16),
            pltpu.VMEM((2, D, WIDE), F32),
            pltpu.SemaphoreType.DMA((n,)),
            pltpu.SemaphoreType.DMA,
            pltpu.SemaphoreType.DMA((2,)),
        ],
        compiler_params=params(),
        name="experts_second" if add_into else "experts_first",
        cost_estimate=pl.CostEstimate(flops=n * 18 * ROWS * D * F, bytes_accessed=n * (24 << 20), transcendentals=n * 2 * ROWS * F),
    )(*operands)


def combine_kernel(base, steps, extras, final, first_ref, *refs):
    cnt_refs = refs[:PAIRS]
    refs = refs[PAIRS:]
    dx_refs = refs[:N_CHUNK]
    dg_refs = refs[N_CHUNK:2 * N_CHUNK]
    refs = refs[2 * N_CHUNK:]
    pos_refs = refs[:steps]
    id_refs = refs[steps:2 * steps]
    extra_refs = refs[2 * steps:2 * steps + extras]
    refs = refs[2 * steps + extras:]
    if final == 2:
        refs = refs[2:]
    if final:
        dx_out, dg_out, sums = refs[:3]
        refs = refs[3:]
    else:
        sums = refs[0]
        refs = refs[1:]
    pick, rows, stage, dg_stage, sem = refs
    step = pl.program_id(0)
    side = lax.rem(step, 2)
    first = first_ref[0]

    def loads(i):
        source = base + 2 * i
        out = []
        for k in range(N_CHUNK):
            for j in range(CHUNKS[k]):
                e = STARTS[k] + j
                place = jnp.int32(0)
                for src in range(SRC - 1):
                    place = place + jnp.where(src < source, count_at(cnt_refs, src, e), 0)
                window = pl.ds(aligned(place), CAP)
                out.append(pltpu.make_async_copy(dx_refs[k].at[j, window, :], stage.at[lax.rem(i, 2), e], sem.at[lax.rem(i, 2)]))
                out.append(pltpu.make_async_copy(dg_refs[k].at[j, window, :], dg_stage.at[lax.rem(i, 2), e], sem.at[lax.rem(i, 2)]))
        return out

    @pl.when(step == 0)
    def _():
        for load in loads(step):
            load.start()
        rows[...] = jnp.zeros((ROWS + TILE, D), BF16)

    @pl.when(step + 1 < steps)
    def _():
        for load in loads(step + 1):
            load.start()

    pos = pos_refs[0][...]
    ids = id_refs[0][...]
    for i in range(1, steps):
        pos = jnp.where(step == i, pos_refs[i][...], pos)
        ids = jnp.where(step == i, id_refs[i][...], ids)
    slots = lax.broadcasted_iota(jnp.int32, (CAP, TOK), 0)
    total = jnp.int32(0)
    starts, counts = [], []
    for e in range(EXP):
        pick[pl.ds(aligned(total), CAP), :] = jnp.where(slots == pos[e:e + 1, :], 1.0, 0.0).astype(BF16)
        starts.append(total)
        here = count_at(cnt_refs, base, e)
        for i in range(1, steps):
            here = jnp.where(step == i, count_at(cnt_refs, base + 2 * i, e), here)
        counts.append(here)
        total = total + counts[e]
    pick[pl.ds(aligned(total), TILE), :] = jnp.zeros((TILE, TOK), BF16)

    for load in loads(step):
        load.wait()
    dg_choice = jnp.zeros((TOP_K, TOK), F32)
    for e in range(EXP):
        block = stage[side, e]
        if e == EXP - 1:
            live = lax.broadcasted_iota(jnp.int32, (CAP, 1), 0) < counts[e]
            block = jnp.where(live, block.astype(F32), 0.0).astype(BF16)
        rows[pl.ds(aligned(starts[e]), CAP), :] = block
        hit = slots == pos[e:e + 1, :]
        dg_tok = jnp.sum(jnp.where(hit, dg_stage[side, e, :, :1], 0.0), axis=0, keepdims=True)
        dg_choice = dg_choice + jnp.where(ids == first + e, dg_tok, 0.0)

    start = jnp.zeros((TOK, D), F32)
    left = dg_choice[:, :D]
    right = dg_choice[:, D:]
    for extra in extra_refs:
        start = start + extra[:TOK, :]
        left = left + extra[TOK:TOK + 8, :]
        right = right + extra[TOK + 8:, :TOK - D]
    sums[:TOK, :] = start

    def body(t, carry):
        part = pl.ds(pl.multiple_of(t * TILE, TILE), TILE)
        sums[:TOK, :] += lax.dot_general(pick[part, :], rows[part, :], (((0,), (0,)), ((), ())), preferred_element_type=F32)
        return carry

    lax.fori_loop(0, (total + (TILE - 1)) // TILE, body, 0)
    if final:
        dx_out[...] = sums[:TOK, :].astype(BF16)
        dg_out[:, :D] = left
        dg_out[:, D:] = right
    else:
        sums[TOK:TOK + 8, :] = left
        sums[TOK + 8:, :] = jnp.zeros((8, D), F32)
        sums[TOK + 8:, :TOK - D] = right


def combine(first, tables, dx_rows, dg_rows, base, steps, partner=None, arrived=(), final=None, mb=0):
    smem = pl.BlockSpec(memory_space=pltpu.SMEM)
    anywhere = pl.BlockSpec(memory_space=pl.ANY)
    block = pl.BlockSpec((None, EXP, TOK), lambda i: (base % 2, 0, 0))
    used = tables[base // 2:base // 2 + steps]
    whole = pl.BlockSpec((SUM_ROWS, D), lambda i: (0, 0))
    extra_specs = [] if partner is None else [pl.BlockSpec((None, SUM_ROWS, D), lambda i: (base // 2, 0, 0))]
    extra_specs += [whole] * len(arrived)
    extra = ([] if partner is None else [partner]) + list(arrived)
    scratch = [
        pltpu.VMEM((ROWS + TILE, TOK), BF16),
        pltpu.VMEM((ROWS + TILE, D), BF16),
        pltpu.VMEM((2, EXP, CAP, D), BF16),
        pltpu.VMEM((2, EXP, CAP, 128), F32),
        pltpu.SemaphoreType.DMA((2,)),
    ]
    in_specs = [smem] * (1 + PAIRS) + [anywhere] * (2 * N_CHUNK) + [block] * (2 * steps) + extra_specs
    operands = [first, *(t[3] for t in tables), *dx_rows, *dg_rows, *(t[0] for t in used), *(t[2] for t in used), *extra]
    mode, aliases = 0, {}
    if final is None:
        if steps > 1:
            outs = jax.ShapeDtypeStruct((steps, SUM_ROWS, D), F32)
            out_specs = pl.BlockSpec((None, SUM_ROWS, D), lambda i: (i, 0, 0))
        else:
            outs, out_specs = jax.ShapeDtypeStruct((SUM_ROWS, D), F32), whole
    else:
        outs = (jax.ShapeDtypeStruct((MICRO, TOK, D), BF16), jax.ShapeDtypeStruct((MICRO, TOP_K, TOK), F32))
        out_specs = (pl.BlockSpec((None, TOK, D), lambda i: (mb, 0, 0)), pl.BlockSpec((None, TOP_K, TOK), lambda i: (mb, 0, 0)))
        scratch = [pltpu.VMEM((TOK, D), F32)] + scratch
        mode = 1
        if final:
            mode = 2
            aliases = {len(operands): 0, len(operands) + 1: 1}
            in_specs += [anywhere, anywhere]
            operands += list(final)
    return pl.pallas_call(
        functools.partial(combine_kernel, base, steps, len(extra), mode),
        grid=(steps,),
        out_shape=outs,
        in_specs=in_specs,
        out_specs=out_specs,
        scratch_shapes=scratch,
        input_output_aliases=aliases,
        compiler_params=params(),
        name="combine",
        cost_estimate=pl.CostEstimate(flops=steps * 2 * ROWS * TOK * D, bytes_accessed=steps * (8 << 20), transcendentals=0),
    )(*operands)


SWAP = [(0, 1), (1, 0)]


def swap(value, axis):
    return lax.ppermute(value, axis, SWAP)


def solution(mesh):
    cube = Mesh(mesh.devices.reshape(2, 2, 2, 2), ('z', 'y', 'x', 'c'))
    tok_spec = P(None, ('z', 'y', 'x', 'c'), None)
    spec_edf = P(('x', 'c'), ('z', 'y'), None)
    spec_efd = P(('x', 'c'), None, ('z', 'y'))

    def gather_tokens(block):
        from_y = swap(block, 'y')
        from_x = swap(block, 'x')
        from_xy = swap(from_y, 'x')
        return [
            block, swap(block, 'c'),
            from_y, swap(from_y, 'c'),
            from_x, swap(from_x, 'c'),
            from_xy, swap(from_xy, 'c'),
        ]

    def local_step(x_in, dy_out, expert_idx, gate_prob, w_one, w_two, w_three):
        z, y, x, c = (lax.axis_index(name) for name in 'zyxc')
        place = jnp.stack([z, y]).astype(jnp.int32)
        first = ((x * 2 + c) * 16 + y * EXP).astype(jnp.int32).reshape(1)
        ids = jnp.swapaxes(expert_idx, 1, 2)
        gate = jnp.swapaxes(gate_prob, 1, 2)

        tokens = [gather_tokens(token_block(x_in, dy_out, ids, gate, mb)) for mb in range(MICRO)]

        w_two_t = jnp.swapaxes(w_two, 1, 2)

        def shard(half, k):
            cut = [lax.dynamic_slice_in_dim(w, half * EXP + STARTS[k], CHUNKS[k], 0) for w in (w_one, w_three, w_two_t)]
            return jnp.concatenate(cut, axis=2)

        pieces = []
        for k in range(N_CHUNK):
            own = shard(y, k)
            from_y = swap(shard(1 - y, k), 'y')
            from_z = swap(own, 'z')
            from_yz = swap(from_y, 'z')
            pieces.append((own, from_y, from_z, from_yz))

        tables, rows = [], []
        for mb in range(MICRO):
            tables.append([routing(first, tokens[mb][2 * p:2 * p + 2]) for p in range(PAIRS)])
            got = None
            for p in range(PAIRS):
                got = gather_rows(tables[mb], tokens[mb], got, p)
            rows.append(got)
        counts = [[table[3] for table in tables[mb]] for mb in range(MICRO)]

        acc, keep, send = [], [], []
        dx_rows, dg_rows = ([], []), ([], [])
        for k in range(N_CHUNK):
            res = run_experts(place, counts[0], rows[0], pieces[k], None, k)
            dx_rows[0].append(res[0])
            dg_rows[0].append(res[1])
            acc.append(res[2])
        for k in range(N_CHUNK):
            res = run_experts(place, counts[1], rows[1], pieces[k], acc[k], k)
            dx_rows[1].append(res[0])
            dg_rows[1].append(res[1])
            keep.append(res[2])
            send.append(res[3])

        done = ()
        for mb in range(MICRO):
            args = (first, tables[mb], dx_rows[mb], dg_rows[mb])
            partner = swap(combine(*args, 1, 4), 'c')
            far = swap(combine(*args, 6, 1, partner), 'x')
            near = swap(combine(*args, 4, 1, partner), 'x')
            last = swap(combine(*args, 2, 1, partner, (far,)), 'y')
            done = combine(*args, 0, 1, partner, (near, last), final=done, mb=mb)

        bufs = [jnp.zeros((2 * EXP, QUARTER, F), F32)] * 3
        for k in range(N_CHUNK):
            other = swap(send[k], 'z')

            def cut(which):
                return lax.dynamic_slice_in_dim(keep[k], which * QUARTER, QUARTER, 1) + lax.dynamic_slice_in_dim(other, which * QUARTER, QUARTER, 1)

            theirs = swap(cut(1 - y), 'y')
            mine = cut(y)
            for part in range(3):
                cols = slice(part * F, (part + 1) * F)
                buf = lax.dynamic_update_slice_in_dim(bufs[part], mine[:, :, cols], y * EXP + STARTS[k], 0)
                bufs[part] = lax.dynamic_update_slice_in_dim(buf, theirs[:, :, cols], (1 - y) * EXP + STARTS[k], 0)

        dx_in, d_gate = done
        return dx_in, jnp.swapaxes(d_gate, 1, 2), bufs[0], jnp.swapaxes(bufs[2], 1, 2), bufs[1]

    return jax.shard_map(
        local_step,
        mesh=cube,
        in_specs=(tok_spec, tok_spec, tok_spec, tok_spec, spec_edf, spec_efd, spec_edf),
        out_specs=(tok_spec, tok_spec, spec_edf, spec_efd, spec_edf),
        check_vma=False,
    )
```
